32 devices in a mesh: ctx: 16 (over z, y, x), grp: 2 (over core).
Axes of the slice: x: 2, y: 2, z: 4, core: 2. Of those that a mesh axis runs over, the one named last changes fastest.
Arguments:
- head_inputs: bfloat16 [32768, 80, 64], P('ctx', 'grp'), may hold values from -6 to 6
- gate_inputs: bfloat16 [32768, 80, 64], P('ctx', 'grp'), may hold values from -6 to 6
- step_raw: float32 [32768, 80], P('ctx', 'grp'), may hold values from -4 to 4
- step_bias: float32 [80], P('grp'), may hold values from -4 to -1
- decay_rate: float32 [80], P('grp'), may hold values from 3.0517578e-05 to 0.03125
- input_proj: bfloat16 [32768, 128], P('ctx'), may hold values from -6 to 6
- output_proj: bfloat16 [32768, 128], P('ctx'), may hold values from -6 to 6
- norm_gain: float32 [80, 64], P('grp'), may hold values from 0.5 to 1.5
Outputs:
- layer_out: bfloat16 [32768, 80, 64], P('ctx', 'grp')
The draws below stay inside these ranges and needn't reach their ends.
All inputs are finite; a program needn't handle non-finite values.
Results may differ from the reference program's by a relative error of at most 0.001.
Values sent between devices are 32-bit elements.
A program may use at most 192 MiB of HBM per device.

```python
import math
import jax
import jax.numpy as jnp
from jax import lax

HEADS = 80
HEAD_DIM = 64
STATE = 128
BLOCK = 256
TOKENS = 32768


def block_scale(stream_key, dims, split, low, largest):
    factor_of = 1.0
    for position, parts in split:
        heights = jax.random.uniform(jax.random.fold_in(jax.random.fold_in(stream_key, 6), position), (parts,), jnp.float32, low / len(split), largest / len(split))
        factor_of = factor_of * jnp.repeat(jnp.exp(heights), dims[position] // parts).reshape((-1,) + (1,) * (len(dims) - 1 - position))
    return factor_of


def gaussian(own_key, dims, scale, most, cuts=(), dtype=jnp.bfloat16):
    array = jax.random.normal(own_key, dims, jnp.float32) * scale
    if len(cuts) > 0:
        array = block_scale(own_key, dims, cuts, -0.22, 0.18) * array
    return jnp.clip(array, min=-most, max=most).astype(dtype)


def setup_inputs(seed: int = 0) -> dict:
    seeds = jax.random.split(jax.random.key(seed), 9)
    return {
        "head_inputs": gaussian(seeds[0], (TOKENS, HEADS, HEAD_DIM), 1.0, 6.0, ((0, 16), (1, 2))),
        "gate_inputs": gaussian(seeds[1], (TOKENS, HEADS, HEAD_DIM), 1.0, 6.0, ((0, 16), (1, 2))),
        "step_raw": gaussian(seeds[2], (TOKENS, HEADS), 1.0, 4.0, ((0, 16), (1, 2)), jnp.float32),
        "step_bias": jnp.clip(-4.0 + 3.0 * jax.random.uniform(seeds[3], (HEADS,), jnp.float32) ** block_scale(seeds[3], (HEADS,), ((0, 2),), -0.2, 0.2), -4.0, -1.0),
        "decay_rate": jnp.clip(jnp.exp(math.log(0.03125) - 6.931472 * jax.random.uniform(seeds[4], (HEADS,), jnp.float32) ** block_scale(seeds[4], (HEADS,), ((0, 2),), -0.2, 0.2)), 3.0517578125e-05, 0.03125),
        "input_proj": gaussian(seeds[5], (TOKENS, STATE), 1.0, 6.0, ((0, 16),)),
        "output_proj": gaussian(seeds[6], (TOKENS, STATE), 1.0, 6.0, ((0, 16),)),
        "norm_gain": jnp.clip(1.0 + 0.1 * jax.random.normal(seeds[7], (HEADS, HEAD_DIM), jnp.float32), 0.5, 1.5),
    }


epsilon = 1e-05

def block_within(scaled, decay_block, proj_in, proj_out):
    running = jnp.cumsum(decay_block, axis=0)
    length = decay_block.shape[0]
    causal = jnp.tril(jnp.ones((length, length), jnp.bool_))
    spread = running[:, None, :] - running[None, :, :]
    weights = jnp.exp(jnp.where(causal[:, :, None], spread, -jnp.inf))
    scores = jnp.dot(proj_out, proj_in.T, preferred_element_type=jnp.float32)
    within = jnp.einsum('tsh,shp->thp', scores[:, :, None] * weights, scaled, precision=lax.Precision.HIGHEST)
    return (running, within)

def block_state(scaled, running, proj_in):
    remain = jnp.exp(running[-1][None, :] - running)
    return jnp.einsum('shp,sn->hpn', scaled * remain[:, :, None], proj_in.astype(jnp.float32), precision=lax.Precision.HIGHEST)

def reference(head_inputs, gate_inputs, step_raw, step_bias, decay_rate, input_proj, output_proj, norm_gain):
    step_size = jax.nn.softplus(step_raw + step_bias)
    log_decay = -decay_rate * step_size
    blocks = TOKENS // BLOCK
    pieces = (head_inputs.reshape(blocks, BLOCK, HEADS, HEAD_DIM), gate_inputs.reshape(blocks, BLOCK, HEADS, HEAD_DIM), step_size.reshape(blocks, BLOCK, HEADS), log_decay.reshape(blocks, BLOCK, HEADS), input_proj.reshape(blocks, BLOCK, STATE), output_proj.reshape(blocks, BLOCK, STATE))

    def advance(current, block_in):
        raw_block, gate_block, step_block, decay_block, proj_in, proj_out = block_in
        scaled = raw_block.astype(jnp.float32) * step_block[:, :, None]
        running, within = block_within(scaled, decay_block, proj_in, proj_out)
        across = jnp.exp(running)[:, :, None] * jnp.einsum('tn,hpn->thp', proj_out.astype(jnp.float32), current, precision=lax.Precision.HIGHEST)
        contrib = block_state(scaled, running, proj_in)
        current = jnp.exp(running[-1])[:, None, None] * current + contrib
        mixed_out = within + across
        gated_out = mixed_out * jax.nn.silu(gate_block.astype(jnp.float32))
        mean_sq = lax.optimization_barrier(jnp.sum(gated_out * gated_out, axis=(1, 2))) / (HEADS * HEAD_DIM)
        result = gated_out * lax.rsqrt(mean_sq + epsilon)[:, None, None] * norm_gain
        return (current, result.astype(jnp.bfloat16))
    start_state = jnp.zeros((HEADS, HEAD_DIM, STATE), jnp.float32)
    last_state, outputs = lax.scan(advance, start_state, pieces)
    return outputs.reshape(TOKENS, HEADS, HEAD_DIM)
```

```python
import functools

import jax
import jax.numpy as jnp
from jax import lax
from jax.experimental import pallas as pl
from jax.experimental.pallas import tpu as pltpu
from jax.sharding import PartitionSpec as P

BLOCK = 256
EPS = 1e-05
NT = (((1,), (1,)), ((), ()))
F32, BF16 = jnp.float32, jnp.bfloat16


def dot(a, b):
    return jnp.dot(a, b, preferred_element_type=F32)


def split(v):
    hi = v.astype(BF16)
    return hi, (v - hi.astype(F32)).astype(BF16)


def decays(raw, bias, rate):
    v = raw + bias
    step = jnp.maximum(v, 0.0) + jnp.log1p(jnp.exp(-jnp.abs(v)))
    log = -rate * step
    q = raw.shape[1]
    upto = lax.broadcasted_iota(jnp.int32, (q, q), 0) <= lax.broadcasted_iota(jnp.int32, (q, q), 1)
    upto = upto.astype(BF16)
    a, rest = log.astype(BF16), log - log.astype(BF16).astype(F32)
    b, c = split(rest)
    running = dot(a, upto) + dot(b, upto) + dot(c, upto)
    return step, running


def scaled_rows(x_ref, w_ref, yhi_ref, ylo_ref, first, group, width):
    for i in range(group):
        h = first + i
        w = w_ref[pl.ds(h, 1), :]
        y = x_ref[pl.ds(pl.multiple_of(h * width, width), width), :].astype(F32) * w
        hi, lo = split(y)
        yhi_ref[i * width:(i + 1) * width, :] = hi
        ylo_ref[i * width:(i + 1) * width, :] = lo


def state_kernel(heads, width, group, x_ref, raw_ref, bias_ref, rate_ref, b_ref,
                 loc_ref, last_ref, log_ref, s_ref, w_ref, e_ref, t_ref, yhi_ref, ylo_ref):
    c = pl.program_id(0)

    @pl.when(c == 0)
    def _():
        s_ref[...] = jnp.zeros_like(s_ref)
        t_ref[...] = jnp.zeros_like(t_ref)

    step, running = decays(raw_ref[...], bias_ref[...], rate_ref[...])
    end = jnp.broadcast_to(running[:, -1:], e_ref.shape)
    w_ref[...] = step * jnp.exp(-running)
    e_ref[...] = jnp.exp(end)
    t_ref[...] += end
    rows = group * width

    def body(g, carry):
        first = g * group
        at = pl.ds(pl.multiple_of(first * width, width), rows)
        scaled_rows(x_ref, w_ref, yhi_ref, ylo_ref, first, group, width)
        part = dot(yhi_ref[...], b_ref[...]) + dot(ylo_ref[...], b_ref[...])
        old = s_ref[at, :]
        loc_ref[0, at, :] = old
        new = old + part
        for i in range(group):
            s_ref[pl.ds(pl.multiple_of((first + i) * width, width), width), :] = (
                new[i * width:(i + 1) * width, :] * e_ref[pl.ds(first + i, 1), :])
        return carry

    lax.fori_loop(0, heads // group, body, 0)
    last_ref[...] = s_ref[...]
    log_ref[...] = t_ref[...]


def output_kernel(heads, width, group, x_ref, gate_ref, raw_ref, bias_ref, rate_ref, b_ref, c_ref,
                  loc_ref, init_ref, out_ref, sq_ref,
                  w_ref, e_ref, t_ref, d_ref, yhi_ref, ylo_ref, shl_ref):
    c = pl.program_id(0)

    @pl.when(c == 0)
    def _():
        t_ref[...] = jnp.zeros_like(t_ref)

    step, running = decays(raw_ref[...], bias_ref[...], rate_ref[...])
    w_ref[...] = step * jnp.exp(-running)
    e_ref[...] = jnp.exp(running)
    d_ref[...] = jnp.exp(t_ref[...])
    t_ref[...] += jnp.broadcast_to(running[:, -1:], t_ref.shape)
    rows = group * width
    q, n = b_ref.shape
    scores = lax.dot_general(b_ref[...], c_ref[...], NT, preferred_element_type=F32)
    causal = lax.broadcasted_iota(jnp.int32, (q, q), 0) <= lax.broadcasted_iota(jnp.int32, (q, q), 1)
    mhi, mlo = split(jnp.where(causal, scores, 0.0))
    twice = jnp.concatenate([c_ref[...], c_ref[...]], axis=1)

    def body(g, total):
        first = g * group
        scaled_rows(x_ref, w_ref, yhi_ref, ylo_ref, first, group, width)
        for i in range(group):
            at = pl.ds(pl.multiple_of((first + i) * width, width), width)
            s = loc_ref[0, at, :] + init_ref[at, :] * d_ref[pl.ds(first + i, 1), :]
            hi, lo = split(s)
            shl_ref[i * width:(i + 1) * width, :n] = hi
            shl_ref[i * width:(i + 1) * width, n:] = lo
        mixed = (dot(yhi_ref[...], mhi) + dot(ylo_ref[...], mhi) + dot(yhi_ref[...], mlo)
                 + lax.dot_general(shl_ref[...], twice, NT, preferred_element_type=F32))
        for i in range(group):
            at = pl.ds(pl.multiple_of((first + i) * width, width), width)
            v = gate_ref[at, :].astype(F32)
            half = 0.5 * v
            silu = half + half * jnp.tanh(half)
            gated = mixed[i * width:(i + 1) * width, :] * e_ref[pl.ds(first + i, 1), :] * silu
            out_ref[at, :] = gated
            total = total + jnp.sum((gated * gated).reshape(width // 8, 8, q), axis=0)
        return total

    total = lax.fori_loop(0, heads // group, body, jnp.zeros((8, q), F32))
    sq_ref[...] = jnp.sum(total, axis=0, keepdims=True)


def group_of(heads, most=10):
    return max(k for k in range(1, most + 1) if heads % k == 0)


def carry(last, logs, width):
    count, here = lax.axis_size("ctx"), lax.axis_index("ctx")
    inner = 4 if count % 4 == 0 else 2 if count % 2 == 0 else 1
    outer = count // inner
    rows, n = last.shape
    heads = logs.shape[0]
    part = rows // inner
    me = here % inner
    parts = last.reshape(inner, part, n)
    wide = [jnp.concatenate([lax.dynamic_index_in_dim(parts, me ^ k, 0, False), logs], 0)
            for k in range(inner)]
    got = [wide[0]] + [
        lax.ppermute(wide[k], "ctx", [(i, i ^ k) for i in range(count)]) for k in range(1, inner)]
    got = jnp.stack(got)

    def spread(log):
        long = jnp.repeat(log, width, axis=0).reshape(inner, part, n)
        return lax.dynamic_index_in_dim(long, me, 0, False)

    before, prefix, since = jnp.zeros((part, n), F32), [], jnp.zeros((heads, n), F32)
    logs_before = []
    for k in range(inner):
        piece = lax.dynamic_index_in_dim(got, me ^ k, 0, False)
        prefix.append(before)
        logs_before.append(since)
        log = piece[part:]
        before = before * jnp.exp(spread(log)) + piece[:part]
        since = since + log
    total, total_log = before, since
    acc = lax.ppermute(jnp.concatenate([total, total_log], 0), "ctx",
                       [(i, i + inner) for i in range(count - inner)])
    shift = 1
    while shift < outer - 1:
        earlier = lax.ppermute(acc, "ctx", [(i, i + shift * inner) for i in range(count - shift * inner)])
        state = acc[:part] + jnp.exp(spread(acc[part:])) * earlier[:part]
        acc = jnp.concatenate([state, acc[part:] + earlier[part:]], 0)
        shift *= 2
    entering = acc[:part]
    finals = jnp.stack([p + jnp.exp(spread(l)) * entering for p, l in zip(prefix, logs_before)])
    mine = [lax.dynamic_index_in_dim(finals, me ^ k, 0, False) for k in range(inner)]
    back = [mine[0]] + [
        lax.ppermute(mine[k], "ctx", [(i, i ^ k) for i in range(count)]) for k in range(1, inner)]
    back = jnp.stack(back)
    return jnp.concatenate([lax.dynamic_index_in_dim(back, me ^ k, 0, False) for k in range(inner)], 0)


def shards(head_inputs, gate_inputs, step_raw, step_bias, decay_rate, input_proj, output_proj, norm_gain):
    tokens, heads, width = head_inputs.shape
    n = input_proj.shape[1]
    rows = heads * width
    blocks = tokens // BLOCK
    group = group_of(heads)
    x = jnp.transpose(head_inputs, (1, 2, 0)).reshape(rows, tokens)
    gate = jnp.transpose(gate_inputs, (1, 2, 0)).reshape(rows, tokens)
    raw = step_raw.T
    bias, rate = step_bias[:, None], decay_rate[:, None]

    wide = pl.BlockSpec((rows, BLOCK), lambda c: (0, c))
    per_head = pl.BlockSpec((heads, BLOCK), lambda c: (0, c))
    whole = lambda *shape: pl.BlockSpec(shape, lambda c: (0,) * len(shape))
    proj = pl.BlockSpec((BLOCK, n), lambda c: (c, 0))
    local = pl.BlockSpec((1, rows, n), lambda c: (c, 0, 0))
    params = pltpu.CompilerParams(dimension_semantics=("arbitrary",), vmem_limit_bytes=60 << 20)
    ys = [pltpu.VMEM((group * width, BLOCK), BF16)] * 2

    loc, last, logs = pl.pallas_call(
        functools.partial(state_kernel, heads, width, group),
        grid=(blocks,),
        in_specs=[wide, per_head, whole(heads, 1), whole(heads, 1), proj],
        out_specs=[local, whole(rows, n), whole(heads, n)],
        out_shape=[jax.ShapeDtypeStruct((blocks, rows, n), F32),
                   jax.ShapeDtypeStruct((rows, n), F32),
                   jax.ShapeDtypeStruct((heads, n), F32)],
        scratch_shapes=[pltpu.VMEM((rows, n), F32), pltpu.VMEM((heads, BLOCK), F32),
                        pltpu.VMEM((heads, n), F32), pltpu.VMEM((heads, n), F32)] + ys,
        compiler_params=params, name="local_state",
    )(x, raw, bias, rate, input_proj)

    init = carry(last, logs, width)

    gated, local_sq = pl.pallas_call(
        functools.partial(output_kernel, heads, width, group),
        grid=(blocks,),
        in_specs=[wide, wide, per_head, whole(heads, 1), whole(heads, 1), proj, proj, local, whole(rows, n)],
        out_specs=[wide, pl.BlockSpec((1, BLOCK), lambda c: (0, c))],
        out_shape=[jax.ShapeDtypeStruct((rows, tokens), F32), jax.ShapeDtypeStruct((1, tokens), F32)],
        scratch_shapes=[pltpu.VMEM((heads, BLOCK), F32), pltpu.VMEM((heads, BLOCK), F32),
                        pltpu.VMEM((heads, n), F32), pltpu.VMEM((heads, n), F32)] + ys
                       + [pltpu.VMEM((group * width, 2 * n), BF16)],
        compiler_params=params, name="outputs",
    )(x, gate, raw, bias, rate, input_proj, output_proj, loc, init)

    total_sq = lax.psum(local_sq, "grp")
    channels = lax.axis_size("grp") * rows
    scale = lax.rsqrt(total_sq / channels + EPS)
    result = (gated * scale * norm_gain.reshape(rows, 1)).astype(BF16)
    return jnp.transpose(result.reshape(heads, width, tokens), (2, 0, 1))


def solution(mesh):
    in_specs = (P("ctx", "grp", None), P("ctx", "grp", None), P("ctx", "grp"), P("grp"), P("grp"),
                P("ctx", None), P("ctx", None), P("grp", None))
    return jax.shard_map(shards, mesh=mesh, in_specs=in_specs, out_specs=P("ctx", "grp", None), check_vma=False)
```

```python
import functools
import math

import jax
import jax.numpy as jnp
from jax import lax
from jax.experimental import pallas as pl
from jax.experimental.pallas import tpu as pltpu
from jax.sharding import PartitionSpec as P

BLOCK = 256
EPS = 1e-05
NT = (((1,), (1,)), ((), ()))
F32, BF16 = jnp.float32, jnp.bfloat16


def dot(a, b):
    return jnp.dot(a, b, preferred_element_type=F32)


def split(v):
    hi = v.astype(BF16)
    return hi, (v - hi.astype(F32)).astype(BF16)


def decays(raw, bias, rate):
    v = raw + bias
    step = jnp.maximum(v, 0.0) + jnp.log1p(jnp.exp(-jnp.abs(v)))
    log = -rate * step
    q = raw.shape[1]
    upto = lax.broadcasted_iota(jnp.int32, (q, q), 0) <= lax.broadcasted_iota(jnp.int32, (q, q), 1)
    upto = upto.astype(BF16)
    a, rest = log.astype(BF16), log - log.astype(BF16).astype(F32)
    b, c = split(rest)
    running = dot(a, upto) + dot(b, upto) + dot(c, upto)
    return step, running


def scaled_rows(x_ref, w_ref, yhi_ref, ylo_ref, first, group, width):
    for h in range(first, first + group):
        at = slice(h * width, (h + 1) * width)
        hi, lo = split(x_ref[at, :].astype(F32) * w_ref[h:h + 1, :])
        yhi_ref[at, :] = hi
        ylo_ref[at, :] = lo


def state_kernel(heads, width, group, x_ref, raw_ref, bias_ref, rate_ref, b_ref,
                 loc_ref, last_ref, log_ref, s_ref, w_ref, e_ref, t_ref, yhi_ref, ylo_ref):
    c = pl.program_id(0)

    @pl.when(c == 0)
    def _():
        s_ref[...] = jnp.zeros_like(s_ref)
        t_ref[...] = jnp.zeros_like(t_ref)

    step, running = decays(raw_ref[...], bias_ref[...], rate_ref[...])
    end = jnp.broadcast_to(running[:, -1:], e_ref.shape)
    w_ref[...] = step * jnp.exp(-running)
    e_ref[...] = jnp.exp(end)
    t_ref[...] += end
    rows = group * width

    b = b_ref[...]
    for first in range(0, heads, group):
        at = slice(first * width, first * width + rows)
        scaled_rows(x_ref, w_ref, yhi_ref, ylo_ref, first, group, width)
        part = dot(yhi_ref[at, :], b) + dot(ylo_ref[at, :], b)
        old = s_ref[at, :]
        loc_ref[0, at, :] = old
        new = old + part
        for i in range(group):
            h = first + i
            s_ref[h * width:(h + 1) * width, :] = new[i * width:(i + 1) * width, :] * e_ref[h:h + 1, :]
    last_ref[...] = s_ref[...]
    log_ref[...] = t_ref[...]


def output_kernel(heads, width, group, x_ref, gate_ref, raw_ref, bias_ref, rate_ref, b_ref, c_ref,
                  loc_ref, init_ref, out_ref, sq_ref,
                  w_ref, e_ref, t_ref, d_ref, yhi_ref, ylo_ref, shl_ref):
    c = pl.program_id(0)

    @pl.when(c == 0)
    def _():
        t_ref[...] = jnp.zeros_like(t_ref)

    step, running = decays(raw_ref[...], bias_ref[...], rate_ref[...])
    w_ref[...] = step * jnp.exp(-running)
    e_ref[...] = jnp.exp(running)
    d_ref[...] = jnp.exp(t_ref[...])
    t_ref[...] += jnp.broadcast_to(running[:, -1:], t_ref.shape)
    rows = group * width
    q, n = b_ref.shape
    scores = lax.dot_general(b_ref[...], c_ref[...], NT, preferred_element_type=F32)
    causal = lax.broadcasted_iota(jnp.int32, (q, q), 0) <= lax.broadcasted_iota(jnp.int32, (q, q), 1)
    mhi, mlo = split(jnp.where(causal, scores, 0.0))
    twice = jnp.concatenate([c_ref[...], c_ref[...]], axis=1)

    total = jnp.zeros((8, q), F32)
    for first in range(0, heads, group):
        block = slice(first * width, first * width + rows)
        scaled_rows(x_ref, w_ref, yhi_ref, ylo_ref, first, group, width)
        for h in range(first, first + group):
            at = slice(h * width, (h + 1) * width)
            hi, lo = split(loc_ref[0, at, :] + init_ref[at, :] * d_ref[h:h + 1, :])
            shl_ref[at, :n] = hi
            shl_ref[at, n:] = lo
        mixed = (dot(yhi_ref[block, :], mhi) + dot(ylo_ref[block, :], mhi) + dot(yhi_ref[block, :], mlo)
                 + lax.dot_general(shl_ref[block, :], twice, NT, preferred_element_type=F32))
        for i in range(group):
            h = first + i
            at = slice(h * width, (h + 1) * width)
            v = gate_ref[at, :].astype(F32)
            half = 0.5 * v
            silu = half + half * jnp.tanh(half)
            gated = mixed[i * width:(i + 1) * width, :] * e_ref[h:h + 1, :] * silu
            out_ref[at, :] = gated
            total = total + jnp.sum((gated * gated).reshape(width // 8, 8, q), axis=0)
    sq_ref[...] = jnp.sum(total, axis=0, keepdims=True)


def group_of(heads, most=5):
    return max(k for k in range(1, most + 1) if heads % k == 0)


def carry_kernel(count, inner, pieces, width, last_ref, log_ref, out_ref,
                 got_ref, dgot_ref, ent_ref, nxt_ref, fin_ref, ret_ref,
                 d_send, d_recv, a_send, a_recv, z_send, z_recv, c_send, c_recv):
    here = lax.axis_index("ctx")
    me, plane, planes = lax.rem(here, inner), here // inner, count // inner
    base = here - me
    part = got_ref.shape[1]
    size = part // pieces
    step = math.gcd(size, width)
    mesh = pl.DeviceIdType.MESH
    to = [base + lax.rem(me + k, inner) for k in range(inner)]
    first, final = plane == 0, plane == planes - 1

    barrier = pltpu.get_barrier_semaphore()
    for k in range(1, inner):
        pl.semaphore_signal(barrier, inc=1, device_id={"ctx": to[k]}, device_id_type=mesh)

    @pl.when(jnp.logical_not(first))
    def _():
        pl.semaphore_signal(barrier, inc=1, device_id={"ctx": here - inner}, device_id_type=mesh)

    @pl.when(jnp.logical_not(final))
    def _():
        pl.semaphore_signal(barrier, inc=1, device_id={"ctx": here + inner}, device_id_type=mesh)

    inside = jnp.logical_and(jnp.logical_not(first), jnp.logical_not(final))
    alone = jnp.logical_and(first, final)

    @pl.when(inside)
    def _():
        pl.semaphore_wait(barrier, inner + 1)

    @pl.when(alone)
    def _():
        pl.semaphore_wait(barrier, inner - 1)

    @pl.when(jnp.logical_not(jnp.logical_or(inside, alone)))
    def _():
        pl.semaphore_wait(barrier, inner)

    def remote(src, dst, send, recv, device):
        return pltpu.make_async_remote_copy(src_ref=src, dst_ref=dst, send_sem=send, recv_sem=recv,
                                            device_id={"ctx": device}, device_id_type=mesh)

    def rows_of(s):
        return pl.ds(s * size, size)

    logs = [remote(log_ref, dgot_ref.at[k], d_send.at[k], d_recv.at[k], to[k]) for k in range(1, inner)]
    for copy in logs:
        copy.start()
    owned = [lax.rem(me + k, inner) * part for k in range(inner)]
    out_copies = {}
    for s in range(pieces):
        for k in range(1, inner):
            out_copies[s, k] = remote(
                last_ref.at[pl.ds(pl.multiple_of(owned[k] + s * size, step), size), :],
                got_ref.at[k, rows_of(s), :], a_send.at[k, s], a_recv.at[k, s], to[k])
            out_copies[s, k].start()
    got_ref[0] = last_ref[pl.ds(pl.multiple_of(owned[0], step), part), :]
    dgot_ref[0] = log_ref[...]

    @pl.when(first)
    def _():
        ent_ref[...] = jnp.zeros_like(ent_ref)

    for copy in logs:
        copy.wait()
    chain, back = [], []
    for s in range(pieces):
        for k in range(1, inner):
            out_copies[s, k].wait()
        link = remote(nxt_ref.at[rows_of(s), :], ent_ref.at[rows_of(s), :],
                      z_send.at[s], z_recv.at[s], here + inner)

        @pl.when(jnp.logical_not(first))
        def _():
            link.wait_recv()

        for r in range(s * size, (s + 1) * size, step):
            at = slice(r, r + step)
            head = (owned[0] + r) // width
            state = ent_ref[at, :]
            for j in range(inner):
                fin_ref[j, at, :] = state
                slot = lax.rem(me - j + inner, inner)
                state = state * jnp.exp(dgot_ref[slot, pl.ds(head, 1), :]) + got_ref[slot, at, :]
            nxt_ref[at, :] = state

        @pl.when(jnp.logical_not(final))
        def _():
            link.start()

        for k in range(1, inner):
            copy = remote(fin_ref.at[lax.rem(me + k, inner), rows_of(s), :], ret_ref.at[k, rows_of(s), :],
                          c_send.at[k, s], c_recv.at[k, s], to[k])
            copy.start()
            back.append(copy)
        chain.append(link)

    out_ref[pl.ds(pl.multiple_of(owned[0], step), part), :] = fin_ref[me]

    @pl.when(jnp.logical_not(final))
    def _():
        for link in chain:
            link.wait_send()

    for copy in back:
        copy.wait()
    for k in range(1, inner):
        owner = lax.rem(me - k + inner, inner)
        out_ref[pl.ds(pl.multiple_of(owner * part, step), part), :] = ret_ref[k]


def carry(last, logs, width):
    count = lax.axis_size("ctx")
    inner = 4 if count % 4 == 0 else 2
    rows, n = last.shape
    part = rows // inner
    pieces = 5 if part % 160 == 0 else 1
    vmem = pl.BlockSpec(memory_space=pltpu.VMEM)
    sems = [pltpu.SemaphoreType.DMA((inner,))] * 2
    sems += [pltpu.SemaphoreType.DMA((inner, pieces))] * 2
    sems += [pltpu.SemaphoreType.DMA((pieces,))] * 2
    sems += [pltpu.SemaphoreType.DMA((inner, pieces))] * 2
    return pl.pallas_call(
        functools.partial(carry_kernel, count, inner, pieces, width),
        out_shape=jax.ShapeDtypeStruct((rows, n), F32),
        in_specs=[vmem, vmem],
        out_specs=vmem,
        scratch_shapes=[pltpu.VMEM((inner, part, n), F32), pltpu.VMEM((inner,) + logs.shape, F32),
                        pltpu.VMEM((part, n), F32), pltpu.VMEM((part, n), F32),
                        pltpu.VMEM((inner, part, n), F32), pltpu.VMEM((inner, part, n), F32)] + sems,
        compiler_params=pltpu.CompilerParams(collective_id=0, has_side_effects=True,
                                             vmem_limit_bytes=40 << 20),
        name="carry",
    )(last, logs)


def shards(head_inputs, gate_inputs, step_raw, step_bias, decay_rate, input_proj, output_proj, norm_gain):
    tokens, heads, width = head_inputs.shape
    n = input_proj.shape[1]
    rows = heads * width
    blocks = tokens // BLOCK
    group = group_of(heads)
    x = jnp.transpose(head_inputs, (1, 2, 0)).reshape(rows, tokens)
    gate = jnp.transpose(gate_inputs, (1, 2, 0)).reshape(rows, tokens)
    raw = step_raw.T
    bias, rate = step_bias[:, None], decay_rate[:, None]

    wide = pl.BlockSpec((rows, BLOCK), lambda c: (0, c))
    per_head = pl.BlockSpec((heads, BLOCK), lambda c: (0, c))
    whole = lambda *shape: pl.BlockSpec(shape, lambda c: (0,) * len(shape))
    proj = pl.BlockSpec((BLOCK, n), lambda c: (c, 0))
    local = pl.BlockSpec((1, rows, n), lambda c: (c, 0, 0))
    params = pltpu.CompilerParams(dimension_semantics=("arbitrary",), vmem_limit_bytes=60 << 20)
    ys = [pltpu.VMEM((rows, BLOCK), BF16)] * 2

    loc, last, logs = pl.pallas_call(
        functools.partial(state_kernel, heads, width, group),
        grid=(blocks,),
        in_specs=[wide, per_head, whole(heads, 1), whole(heads, 1), proj],
        out_specs=[local, whole(rows, n), whole(heads, n)],
        out_shape=[jax.ShapeDtypeStruct((blocks, rows, n), F32),
                   jax.ShapeDtypeStruct((rows, n), F32),
                   jax.ShapeDtypeStruct((heads, n), F32)],
        scratch_shapes=[pltpu.VMEM((rows, n), F32), pltpu.VMEM((heads, BLOCK), F32),
                        pltpu.VMEM((heads, n), F32), pltpu.VMEM((heads, n), F32)] + ys,
        compiler_params=params, name="local_state",
    )(x, raw, bias, rate, input_proj)

    init = carry(last, logs, width)

    gated, local_sq = pl.pallas_call(
        functools.partial(output_kernel, heads, width, group),
        grid=(blocks,),
        in_specs=[wide, wide, per_head, whole(heads, 1), whole(heads, 1), proj, proj, local, whole(rows, n)],
        out_specs=[wide, pl.BlockSpec((1, BLOCK), lambda c: (0, c))],
        out_shape=[jax.ShapeDtypeStruct((rows, tokens), F32), jax.ShapeDtypeStruct((1, tokens), F32)],
        scratch_shapes=[pltpu.VMEM((heads, BLOCK), F32), pltpu.VMEM((heads, BLOCK), F32),
                        pltpu.VMEM((heads, n), F32), pltpu.VMEM((heads, n), F32)] + ys
                       + [pltpu.VMEM((rows, 2 * n), BF16)],
        compiler_params=params, name="outputs",
    )(x, gate, raw, bias, rate, input_proj, output_proj, loc, init)

    total_sq = lax.psum(local_sq, "grp")
    channels = lax.axis_size("grp") * rows
    scale = lax.rsqrt(total_sq / channels + EPS)
    result = (gated * scale * norm_gain.reshape(rows, 1)).astype(BF16)
    return jnp.transpose(result.reshape(heads, width, tokens), (2, 0, 1))


def solution(mesh):
    in_specs = (P("ctx", "grp", None), P("ctx", "grp", None), P("ctx", "grp"), P("grp"), P("grp"),
                P("ctx", None), P("ctx", None), P("grp", None))
    return jax.shard_map(shards, mesh=mesh, in_specs=in_specs, out_specs=P("ctx", "grp", None), check_vma=False)
```

```python
import functools
import math

import jax
import jax.numpy as jnp
from jax import lax
from jax.experimental import pallas as pl
from jax.experimental.pallas import tpu as pltpu
from jax.sharding import PartitionSpec as P

BLOCK = 256
EPS = 1e-05
NT = (((1,), (1,)), ((), ()))
F32, BF16 = jnp.float32, jnp.bfloat16


def dot(a, b):
    return jnp.dot(a, b, preferred_element_type=F32)


def split(v):
    hi = v.astype(BF16)
    return hi, (v - hi.astype(F32)).astype(BF16)


def decays(raw, bias, rate):
    v = raw + bias
    step = jnp.maximum(v, 0.0) + jnp.log1p(jnp.exp(-jnp.abs(v)))
    log = -rate * step
    q = raw.shape[1]
    upto = lax.broadcasted_iota(jnp.int32, (q, q), 0) <= lax.broadcasted_iota(jnp.int32, (q, q), 1)
    upto = upto.astype(BF16)
    a, rest = log.astype(BF16), log - log.astype(BF16).astype(F32)
    b, c = split(rest)
    running = dot(a, upto) + dot(b, upto) + dot(c, upto)
    return step, running


def scaled_rows(x_ref, w_ref, now, yhi_ref, ylo_ref, first, group, width):
    for h in range(first, first + group):
        at = slice(h * width, (h + 1) * width)
        hi, lo = split(x_ref[at, :].astype(F32) * w_ref[h:h + 1, now])
        yhi_ref[at, :] = hi
        ylo_ref[at, :] = lo


def state_kernel(heads, width, group, x_ref, raw_ref, head_ref, b_ref,
                 loc_ref, last_ref, log_ref, w_ref, e_ref, reach_ref,
                 s_ref, end_ref, yhi_ref, ylo_ref):
    c = pl.program_id(0)
    q, n = b_ref.shape

    @pl.when(c == 0)
    def _():
        s_ref[...] = jnp.zeros_like(s_ref)
        since = jnp.zeros((heads, 1), F32)
        for k in range(pl.num_programs(0)):
            at = slice(k * q, (k + 1) * q)
            step, running = decays(raw_ref[:, at], head_ref[:, :1], head_ref[:, 1:])
            w_ref[:, at] = step * jnp.exp(-running)
            e_ref[:, at] = jnp.exp(running)
            reach_ref[:, at] = jnp.exp(running + since)
            end_ref[k] = jnp.exp(jnp.broadcast_to(running[:, -1:], (heads, n)))
            since = since + running[:, -1:]
        log_ref[...] = jnp.broadcast_to(since, log_ref.shape)

    b = b_ref[...]
    rows = group * width
    now = pl.ds(pl.multiple_of(c * q, q), q)
    for first in range(0, heads, group):
        at = slice(first * width, first * width + rows)
        scaled_rows(x_ref, w_ref, now, yhi_ref, ylo_ref, first, group, width)
        part = dot(yhi_ref[at, :], b) + dot(ylo_ref[at, :], b)
        old = s_ref[at, :]
        loc_ref[0, at, :] = old
        new = old + part
        for i in range(group):
            h = first + i
            s_ref[h * width:(h + 1) * width, :] = new[i * width:(i + 1) * width, :] * end_ref[c, h:h + 1, :]
    last_ref[...] = s_ref[...]


def group_of(heads, most=5):
    return max(k for k in range(1, most + 1) if heads % k == 0)


def output_kernel(count, others, inner, pieces, heads, width, group, blocks,
                  x_ref, gate_ref, w_ref, e_ref, reach_ref, b_ref, c_ref, loc_ref, last_ref, log_ref, gain_ref,
                  res_ref,
                  part_ref, yhi_ref, ylo_ref, shl_ref, init_ref, sq_ref, sqgot_ref,
                  got_ref, dgot_ref, ent_ref, nxt_ref, fin_ref, ret_ref,
                  d_send, d_recv, a_send, a_recv, z_send, z_recv, c_send, c_recv, g_send, g_recv):
    t = pl.program_id(0)
    core = lax.axis_index("grp")
    q, n = b_ref.shape
    rows = group * width
    here = lax.axis_index("ctx")
    me, plane, planes = lax.rem(here, inner), here // inner, count // inner
    base = here - me
    part = got_ref.shape[1]
    size = part // pieces
    step = math.gcd(size, width)
    mesh = pl.DeviceIdType.MESH
    to = [base + lax.rem(me + k, inner) for k in range(inner)]
    first, final = plane == 0, plane == planes - 1

    def remote(src, dst, send, recv, device):
        return pltpu.make_async_remote_copy(src_ref=src, dst_ref=dst, send_sem=send, recv_sem=recv,
                                            device_id={"ctx": device}, device_id_type=mesh)

    def rows_of(s):
        return pl.ds(s * size, size)

    owned = [lax.rem(me + k, inner) * part for k in range(inner)]
    logs = [remote(log_ref, dgot_ref.at[k], d_send.at[k], d_recv.at[k], to[k]) for k in range(1, inner)]

    def outgoing(s, k):
        return remote(last_ref.at[pl.ds(pl.multiple_of(owned[k] + s * size, step), size), :],
                      got_ref.at[k, rows_of(s), :], a_send.at[k, s], a_recv.at[k, s], to[k])

    def link_of(s):
        return remote(nxt_ref.at[rows_of(s), :], ent_ref.at[rows_of(s), :],
                      z_send.at[s], z_recv.at[s], here + inner)

    def returning(s, k):
        return remote(fin_ref.at[lax.rem(me + k, inner), rows_of(s), :], ret_ref.at[k, rows_of(s), :],
                      c_send.at[k, s], c_recv.at[k, s], to[k])

    def partner(k, c):
        return pltpu.make_async_remote_copy(
            src_ref=sq_ref.at[c], dst_ref=sqgot_ref.at[k, c], send_sem=g_send.at[k, c], recv_sem=g_recv.at[k, c],
            device_id={"grp": lax.rem(core + k, others)}, device_id_type=mesh)

    @pl.when(t == 0)
    def _():
        barrier = pltpu.get_barrier_semaphore()
        for k in range(1, inner):
            pl.semaphore_signal(barrier, inc=1, device_id={"ctx": to[k]}, device_id_type=mesh)

        for k in range(1, others):
            pl.semaphore_signal(barrier, inc=1, device_id={"grp": lax.rem(core + k, others)}, device_id_type=mesh)

        @pl.when(jnp.logical_not(first))
        def _():
            pl.semaphore_signal(barrier, inc=1, device_id={"ctx": here - inner}, device_id_type=mesh)

        @pl.when(jnp.logical_not(final))
        def _():
            pl.semaphore_signal(barrier, inc=1, device_id={"ctx": here + inner}, device_id_type=mesh)

        inside = jnp.logical_and(jnp.logical_not(first), jnp.logical_not(final))
        alone = jnp.logical_and(first, final)

        @pl.when(inside)
        def _():
            pl.semaphore_wait(barrier, inner + others)

        @pl.when(alone)
        def _():
            pl.semaphore_wait(barrier, inner + others - 2)

        @pl.when(jnp.logical_not(jnp.logical_or(inside, alone)))
        def _():
            pl.semaphore_wait(barrier, inner + others - 1)

        for copy in logs:
            copy.start()
        for s in range(pieces):
            for k in range(1, inner):
                outgoing(s, k).start()
        got_ref[0] = last_ref[pl.ds(pl.multiple_of(owned[0], step), part), :]
        dgot_ref[0] = log_ref[...]

        @pl.when(first)
        def _():
            ent_ref[...] = jnp.zeros_like(ent_ref)

    @pl.when(t < blocks)
    def _():
        scores = lax.dot_general(b_ref[...], c_ref[...], NT, preferred_element_type=F32)
        causal = lax.broadcasted_iota(jnp.int32, (q, q), 0) <= lax.broadcasted_iota(jnp.int32, (q, q), 1)
        mhi, mlo = split(jnp.where(causal, scores, 0.0))
        twice = jnp.concatenate([c_ref[...], c_ref[...]], axis=1)
        for lead in range(0, heads, group):
            block = slice(lead * width, lead * width + rows)
            scaled_rows(x_ref, w_ref, slice(None), yhi_ref, ylo_ref, lead, group, width)
            hi, lo = split(loc_ref[0, block, :])
            shl_ref[block, :n] = hi
            shl_ref[block, n:] = lo
            part_ref[t, block, :] = (
                dot(yhi_ref[block, :], mhi) + dot(ylo_ref[block, :], mhi) + dot(yhi_ref[block, :], mlo)
                + lax.dot_general(shl_ref[block, :], twice, NT, preferred_element_type=F32))

    def exchange(s):
        if s == 0:
            for copy in logs:
                copy.wait()
        for k in range(1, inner):
            outgoing(s, k).wait()

        @pl.when(jnp.logical_not(first))
        def _():
            link_of(s).wait_recv()

        for r in range(s * size, (s + 1) * size, step):
            at = slice(r, r + step)
            head = (owned[0] + r) // width
            state = ent_ref[at, :]
            for j in range(inner):
                fin_ref[j, at, :] = state
                slot = lax.rem(me - j + inner, inner)
                state = state * jnp.exp(dgot_ref[slot, pl.ds(head, 1), :]) + got_ref[slot, at, :]
            nxt_ref[at, :] = state

        @pl.when(jnp.logical_not(final))
        def _():
            link_of(s).start()

        for k in range(1, inner):
            returning(s, k).start()

    for s in range(pieces):
        @pl.when(t == min(2 * s + 1 - s // 2, blocks - 1))
        def _():
            exchange(s)

    @pl.when(t == blocks)
    def _():
        @pl.when(jnp.logical_not(final))
        def _():
            for s in range(pieces):
                link_of(s).wait_send()

        for s in range(pieces):
            for k in range(1, inner):
                returning(s, k).wait()
        for k in range(inner):
            owner = lax.rem(me - k + inner, inner)
            hi, lo = split(fin_ref[me] if k == 0 else ret_ref[k])
            at = pl.ds(pl.multiple_of(owner * part, step), part)
            init_ref[at, :n] = hi
            init_ref[at, n:] = lo

    @pl.when(jnp.logical_and(t >= blocks, t < 2 * blocks))
    def _():
        now = t - blocks
        twice = jnp.concatenate([c_ref[...], c_ref[...]], axis=1)
        total = jnp.zeros((8, q), F32)
        for lead in range(0, heads, group):
            block = slice(lead * width, lead * width + rows)
            entered = lax.dot_general(init_ref[block, :], twice, NT, preferred_element_type=F32)
            for i in range(group):
                h = lead + i
                at = slice(h * width, (h + 1) * width)
                half = 0.5 * gate_ref[at, :].astype(F32)
                silu = half + half * jnp.tanh(half)
                gated = (part_ref[now, at, :] * e_ref[h:h + 1, :]
                         + entered[i * width:(i + 1) * width, :] * reach_ref[h:h + 1, :]) * silu
                part_ref[now, at, :] = gated
                total = total + jnp.sum((gated * gated).reshape(width // 8, 8, q), axis=0)
        sq_ref[now] = jnp.broadcast_to(jnp.sum(total, axis=0, keepdims=True), (8, q))
        for k in range(1, others):
            partner(k, now).start()

    @pl.when(t > blocks)
    def _():
        past = t - blocks - 1
        for k in range(1, others):
            partner(k, past).wait()
        total = sq_ref[past]
        for k in range(1, others):
            total = total + sqgot_ref[k, past]
        scale = lax.rsqrt(total[:1, :] / (others * heads * width) + EPS)
        for lead in range(0, heads, group):
            block = slice(lead * width, lead * width + rows)
            res_ref[block, :] = (part_ref[past, block, :] * scale * gain_ref[block, :]).astype(BF16)


def shards(head_inputs, gate_inputs, step_raw, step_bias, decay_rate, input_proj, output_proj, norm_gain):
    tokens, heads, width = head_inputs.shape
    n = input_proj.shape[1]
    rows = heads * width
    blocks = tokens // BLOCK
    group = group_of(heads)
    x = jnp.transpose(head_inputs, (1, 2, 0)).reshape(rows, tokens)
    gate = jnp.transpose(gate_inputs, (1, 2, 0)).reshape(rows, tokens)
    raw = step_raw.T
    per = jnp.stack([step_bias, decay_rate], axis=1)

    wide = pl.BlockSpec((rows, BLOCK), lambda c: (0, c))
    whole = lambda *shape: pl.BlockSpec(shape, lambda c: (0,) * len(shape))
    proj = pl.BlockSpec((BLOCK, n), lambda c: (c, 0))
    local = pl.BlockSpec((1, rows, n), lambda c: (c, 0, 0))
    params = pltpu.CompilerParams(dimension_semantics=("arbitrary",), vmem_limit_bytes=60 << 20)
    ys = [pltpu.VMEM((rows, BLOCK), BF16)] * 2

    loc, last, logs, w, e, reach = pl.pallas_call(
        functools.partial(state_kernel, heads, width, group),
        grid=(blocks,),
        in_specs=[wide, whole(heads, tokens), whole(heads, 2), proj],
        out_specs=[local, whole(rows, n), whole(heads, n)] + [whole(heads, tokens)] * 3,
        out_shape=[jax.ShapeDtypeStruct((blocks, rows, n), F32),
                   jax.ShapeDtypeStruct((rows, n), F32),
                   jax.ShapeDtypeStruct((heads, n), F32)]
                  + [jax.ShapeDtypeStruct((heads, tokens), F32)] * 3,
        scratch_shapes=[pltpu.VMEM((rows, n), F32), pltpu.VMEM((blocks, heads, n), F32)] + ys,
        compiler_params=params, name="local_state",
    )(x, raw, per, input_proj)

    count, others = lax.axis_size("ctx"), lax.axis_size("grp")
    inner = 4 if count % 4 == 0 else 2
    part = rows // inner
    pieces = 5 if part % 160 == 0 else 1
    early = lambda t: jnp.minimum(t, blocks - 1)
    late = lambda t: jnp.clip(t - blocks, 0, blocks - 1)
    both = lambda t: lax.rem(jnp.minimum(t, 2 * blocks - 1), blocks)
    sems = [pltpu.SemaphoreType.DMA((inner,))] * 2
    sems += [pltpu.SemaphoreType.DMA((inner, pieces))] * 2
    sems += [pltpu.SemaphoreType.DMA((pieces,))] * 2
    sems += [pltpu.SemaphoreType.DMA((inner, pieces))] * 2
    sems += [pltpu.SemaphoreType.DMA((others, blocks))] * 2
    result = pl.pallas_call(
        functools.partial(output_kernel, count, others, inner, pieces, heads, width, group, blocks),
        grid=(2 * blocks + 1,),
        in_specs=[pl.BlockSpec((rows, BLOCK), lambda t: (0, early(t))),
                  pl.BlockSpec((rows, BLOCK), lambda t: (0, late(t))),
                  pl.BlockSpec((heads, BLOCK), lambda t: (0, early(t))),
                  pl.BlockSpec((heads, BLOCK), lambda t: (0, late(t))),
                  pl.BlockSpec((heads, BLOCK), lambda t: (0, late(t))),
                  pl.BlockSpec((BLOCK, n), lambda t: (early(t), 0)),
                  pl.BlockSpec((BLOCK, n), lambda t: (both(t), 0)),
                  pl.BlockSpec((1, rows, n), lambda t: (early(t), 0, 0)),
                  pl.BlockSpec(memory_space=pltpu.VMEM), pl.BlockSpec(memory_space=pltpu.VMEM),
                  whole(rows, 1)],
        out_specs=pl.BlockSpec((rows, BLOCK), lambda t: (0, jnp.clip(t - blocks - 1, 0, blocks - 1))),
        out_shape=jax.ShapeDtypeStruct((rows, tokens), BF16),
        scratch_shapes=[pltpu.VMEM((blocks, rows, BLOCK), F32)] + ys
                       + [pltpu.VMEM((rows, 2 * n), BF16), pltpu.VMEM((rows, 2 * n), BF16),
                          pltpu.VMEM((blocks, 8, BLOCK), F32), pltpu.VMEM((others, blocks, 8, BLOCK), F32),
                          pltpu.VMEM((inner, part, n), F32), pltpu.VMEM((inner, heads, n), F32),
                          pltpu.VMEM((part, n), F32), pltpu.VMEM((part, n), F32),
                          pltpu.VMEM((inner, part, n), F32), pltpu.VMEM((inner, part, n), F32)] + sems,
        compiler_params=pltpu.CompilerParams(dimension_semantics=("arbitrary",), collective_id=0,
                                             has_side_effects=True, vmem_limit_bytes=60 << 20),
        name="outputs",
    )(x, gate, w, e, reach, input_proj, output_proj, loc, last, logs, norm_gain.reshape(rows, 1))
    return jnp.transpose(result.reshape(heads, width, tokens), (2, 0, 1))


def solution(mesh):
    in_specs = (P("ctx", "grp", None), P("ctx", "grp", None), P("ctx", "grp"), P("grp"), P("grp"),
                P("ctx", None), P("ctx", None), P("grp", None))
    return jax.shard_map(shards, mesh=mesh, in_specs=in_specs, out_specs=P("ctx", "grp", None), check_vma=False)
```
